32 devices in a mesh: dp: 2 (over x), section: 4 (over y, core), tensor: 4 (over z).
Axes of the slice: x: 2, y: 2, z: 4, core: 2. Of those that a mesh axis runs over, the one named last changes fastest.
Arguments:
- failed_section: int32 [2], P('dp'), may hold values from 0 to 999
- token_ids: int32 [2, 2048], P('dp'), may hold values from 0 to 100001, as said below
- section_outputs: bfloat16 [2, 4, 2048, 2048], P('dp', 'section', None, 'tensor'), may hold values from -11 to 11
- w_query: float32 [4, 2048, 1024], P('section', 'dp', 'tensor'), may hold values from -1 to 1
- w_key: float32 [4, 2048, 1024], P('section', 'dp', 'tensor'), may hold values from -2 to 2
- w_value: float32 [4, 2048, 1024], P('section', 'dp', 'tensor'), may hold values from -0.125 to 0.125
- w_out: float32 [4, 2048, 1024], P('section', 'dp', 'tensor'), may hold values from -0.75 to 0.75
- m_value: float32 [4, 2048, 1024], P('section', 'dp', 'tensor'), may hold values from -3 to 3
- v_value: float32 [4, 2048, 1024], P('section', 'dp', 'tensor'), may hold values from 0.001 to 1
- m_out: float32 [4, 2048, 1024], P('section', 'dp', 'tensor'), may hold values from -3 to 3
- v_out: float32 [4, 2048, 1024], P('section', 'dp', 'tensor'), may hold values from 0.001 to 1
Outputs:
- restored_query: float32 [2, 4, 2048, 1024], P('dp', 'section', None, 'tensor')
- restored_key: float32 [2, 4, 2048, 1024], P('dp', 'section', None, 'tensor')
- restored_value: float32 [2, 4, 2048, 1024], P('dp', 'section', None, 'tensor')
- restored_out: float32 [2, 4, 2048, 1024], P('dp', 'section', None, 'tensor')
- restored_m_value: float32 [2, 4, 2048, 1024], P('dp', 'section', None, 'tensor')
- restored_v_value: float32 [2, 4, 2048, 1024], P('dp', 'section', None, 'tensor')
- restored_m_out: float32 [2, 4, 2048, 1024], P('dp', 'section', None, 'tensor')
- restored_v_out: float32 [2, 4, 2048, 1024], P('dp', 'section', None, 'tensor')
- attn_update: bfloat16 [2, 4, 2048, 2048], P('dp', 'section', None, 'tensor')
The draws below stay inside these ranges and needn't reach their ends.
Inputs may be any that keep to these rules, and one draw needn't show every extreme that they name: `token_ids`: token ids of each replica's micro-batch; the id 100001 ends a document, the others are ordinary tokens below 100000.
All inputs are finite; a program needn't handle non-finite values.
Results may differ from the reference program's by a relative error of at most 0.0087.
Values may be sent and summed in bfloat16 or wider, within the bound.
No kernel may reach another device: no remote copies, remote signals or barrier semaphores. Data moves between devices by JAX's collectives and lax.ppermute only.
A program may use at most 128 MiB of HBM per device.

```python
import math
import jax
import jax.numpy as jnp
from jax import lax

D = 2048
HD = 128
HEADS = 8
TOKENS = 2048
INNER = 1024
REPLICAS = 2
SECTIONS = 4


def draw_token_ids(key, part):
    word_ids = jax.random.randint(jax.random.fold_in(key, 11), (REPLICAS, TOKENS), 0, 100000)
    doc_marks = jax.random.randint(jax.random.fold_in(key, 12), (REPLICAS, TOKENS), 0, max(2, TOKENS // 8))
    return jnp.where(doc_marks == 0, 100001, word_ids).astype(jnp.int32)


def draw_section_outputs(key, part):
    full_shape = (REPLICAS, SECTIONS, TOKENS, D)
    entries = jnp.clip(jax.random.normal(jax.random.fold_in(key, 23), full_shape, jnp.float32), -6.0, 6.0)
    return entries.astype(jnp.bfloat16)


def projection_pair(key):
    full_shape = (SECTIONS, D, INNER)
    leading = jnp.clip(jax.random.normal(jax.random.fold_in(key, 31), full_shape, jnp.float32), -6.0, 6.0) / math.sqrt(D)
    other = jnp.clip(jax.random.normal(jax.random.fold_in(key, 32), full_shape, jnp.float32), -6.0, 6.0) / math.sqrt(D)
    second = other
    return (leading, second)


def draw_w_query(key, part):
    return projection_pair(key)[0].astype(jnp.float32)


def draw_w_key(key, part):
    return projection_pair(key)[1].astype(jnp.float32)


def block_levels(rng, dims, pieces, least, top_value):
    level, own = 1.0, jax.random.fold_in(rng, 6)
    for dim, parts in pieces:
        draws = jnp.exp(jax.random.uniform(jax.random.fold_in(own, dim), (parts,), jnp.float32, least / len(pieces), top_value / len(pieces)))
        level = level * jnp.repeat(draws, dims[dim] // parts).reshape([-1 if axis == dim else 1 for axis in range(len(dims))])
    return level


def bell_draw(rng, shape, deviation, limit, cuts=(), held_as=jnp.bfloat16):
    drawn = jax.random.normal(rng, shape, jnp.float32) * deviation
    if len(cuts) > 0:
        drawn = block_levels(rng, shape, cuts, -0.22, 0.18) * drawn
    return jnp.clip(drawn, min=-limit, max=limit).astype(held_as)


def setup_inputs(seed: int = 0) -> dict:
    arg_keys = jax.random.split(jax.random.key(seed), 12)
    return {
        "failed_section": jax.random.randint(arg_keys[0], (REPLICAS,), 0, 1000).astype(jnp.int32),
        "token_ids": draw_token_ids(jax.random.fold_in(arg_keys[11], 71), 0),
        "section_outputs": draw_section_outputs(jax.random.fold_in(arg_keys[11], 71), 0),
        "w_query": draw_w_query(jax.random.fold_in(arg_keys[11], 71), 0),
        "w_key": draw_w_key(jax.random.fold_in(arg_keys[11], 71), 0),
        "w_value": bell_draw(arg_keys[5], (SECTIONS, D, INNER), D ** -0.5, 0.125, ((0, 4), (1, 2), (2, 4)), jnp.float32),
        "w_out": bell_draw(arg_keys[6], (SECTIONS, D, INNER), (INNER // 16) ** -0.5, 0.75, ((0, 4), (1, 2), (2, 4)), jnp.float32),
        "m_value": bell_draw(arg_keys[7], (SECTIONS, D, INNER), 0.5, 3.0, ((0, 4), (1, 2), (2, 4)), jnp.float32),
        "v_value": jnp.clip(jnp.exp(math.log(1.0) - 6.9077552 * jax.random.uniform(arg_keys[8], (SECTIONS, D, INNER), jnp.float32) ** block_levels(arg_keys[8], (SECTIONS, D, INNER), ((0, 4), (1, 2), (2, 4)), -0.2, 0.2)), 0.001, 1.0),
        "m_out": bell_draw(arg_keys[9], (SECTIONS, D, INNER), 0.5, 3.0, ((0, 4), (1, 2), (2, 4)), jnp.float32),
        "v_out": jnp.clip(jnp.exp(math.log(1.0) - 6.9077552 * jax.random.uniform(arg_keys[10], (SECTIONS, D, INNER), jnp.float32) ** block_levels(arg_keys[10], (SECTIONS, D, INNER), ((0, 4), (1, 2), (2, 4)), -0.2, 0.2)), 0.001, 1.0),
    }


end_token = 100001
mask_fill = -1e+30

def document_ids(token_row):
    doc_ends = (token_row == end_token).astype(jnp.int32)
    return jnp.cumsum(doc_ends) - doc_ends

def attend_head(query_head, key_head, value_head, allowed):
    scores = jnp.dot(query_head, key_head.T, preferred_element_type=jnp.float32) * (1.0 / math.sqrt(HD))
    scores = jnp.where(allowed, scores, mask_fill)
    highest = lax.optimization_barrier(jnp.max(scores, axis=1, keepdims=True))
    weights = jnp.exp(scores - highest)
    probs = (weights / lax.optimization_barrier(jnp.sum(weights, axis=1, keepdims=True))).astype(jnp.bfloat16)
    return jnp.dot(probs, value_head, preferred_element_type=jnp.float32).astype(jnp.bfloat16)

def recompute(incoming, token_row, query_master, key_master, value_master, out_master):
    queries = jnp.dot(incoming, query_master.astype(jnp.bfloat16), preferred_element_type=jnp.float32).astype(jnp.bfloat16)
    key_vals = jnp.dot(incoming, key_master.astype(jnp.bfloat16), preferred_element_type=jnp.float32).astype(jnp.bfloat16)
    value_vals = jnp.dot(incoming, value_master.astype(jnp.bfloat16), preferred_element_type=jnp.float32).astype(jnp.bfloat16)
    query_heads = queries.reshape(TOKENS, HEADS, HD).transpose(1, 0, 2)
    key_heads = key_vals.reshape(TOKENS, HEADS, HD).transpose(1, 0, 2)
    value_heads = value_vals.reshape(TOKENS, HEADS, HD).transpose(1, 0, 2)
    document = document_ids(token_row)
    positions = jnp.arange(TOKENS)
    allowed = (positions[None, :] <= positions[:, None]) & (document[None, :] == document[:, None])
    context = lax.map(lambda trio: attend_head(trio[0], trio[1], trio[2], allowed), (query_heads, key_heads, value_heads))
    context = context.transpose(1, 0, 2).reshape(TOKENS, INNER)
    return jnp.dot(context, out_master.astype(jnp.bfloat16).T, preferred_element_type=jnp.float32).astype(jnp.bfloat16)

def reference(failed_section, token_ids, section_outputs, w_query, w_key, w_value, w_out, m_value, v_value, m_out, v_out):
    sources = (w_query, w_key, w_value, w_out, m_value, v_value, m_out, v_out)
    results = [jnp.zeros((REPLICAS, SECTIONS, D, INNER), jnp.float32) for item in sources]
    update_all = jnp.zeros((REPLICAS, SECTIONS, TOKENS, D), jnp.bfloat16)
    for replica in range(REPLICAS):
        section_failed = jnp.remainder(failed_section[replica], SECTIONS).astype(jnp.int32)
        before = jnp.remainder(section_failed + SECTIONS - 1, SECTIONS).astype(jnp.int32)
        incoming = section_outputs[replica, before]
        blocks = [source[section_failed] for source in sources]
        update = recompute(incoming, token_ids[replica], blocks[0], blocks[1], blocks[2], blocks[3])
        results = [result.at[replica, section_failed].set(block) for result, block in zip(results, blocks)]
        update_all = update_all.at[replica, section_failed].set(update)
    return (results[0], results[1], results[2], results[3], results[4], results[5], results[6], results[7], update_all)
```

```python
import functools
import math

import jax
import jax.numpy as jnp
from jax import lax
from jax.experimental import pallas as pl
from jax.experimental.pallas import tpu as pltpu
from jax.sharding import PartitionSpec as P

HD = 128
CHUNKS = 2

end_token = 100001
mask_fill = -1e30


def passed_along(array, axis, by):
    count = lax.axis_size(axis)
    return lax.ppermute(array, axis, [(i, (i + by) % count) for i in range(count)])


def swapped(array):
    count = lax.axis_size("section")
    return lax.ppermute(array, "section", [(i, i ^ 1) for i in range(count)])


def document_starts(token_row):
    positions = jnp.arange(token_row.shape[0], dtype=jnp.int32)
    ends = jnp.where(token_row == end_token, positions + 1, 0)
    opens = jnp.concatenate([jnp.zeros((1,), jnp.int32), ends[:-1]])
    return lax.cummax(opens)


def attend_body(info, queries, starts, *rest, pieces, rows, heads):
    kvs, out = rest[:pieces], rest[pieces]
    tops, sums, accs = rest[pieces + 1 :]
    step = pl.program_id(0)
    piece_rows = kvs[0].shape[0]
    width = heads * HD
    first = info[0] + step * rows
    lowest = info[1 + step]
    factor = math.log2(math.e) / math.sqrt(HD)
    row_pos = first + lax.broadcasted_iota(jnp.int32, (rows, piece_rows), 0)
    col = lax.broadcasted_iota(jnp.int32, (rows, piece_rows), 1)
    row_start = starts[...]

    for piece in range(pieces):
        base = info[1 + pl.num_programs(0) + piece]

        def visit(piece=piece, base=base):
            key_pos = col + base
            allowed = (key_pos <= row_pos) & (key_pos >= row_start)
            for head in range(heads):
                span = slice(head * HD, (head + 1) * HD)
                scores = lax.dot_general(
                    queries[:, span], kvs[piece][:, span], (((1,), (1,)), ((), ())),
                    preferred_element_type=jnp.float32,
                )
                scores = jnp.where(allowed, scores * factor, mask_fill)
                top = jnp.max(scores, axis=1, keepdims=True)
                if piece == 0:
                    weights = jnp.exp2(scores - top)
                    sums[head] = jnp.sum(weights, axis=1, keepdims=True)
                    accs[head] = jnp.dot(
                        weights.astype(jnp.bfloat16), kvs[piece][:, width + head * HD : width + (head + 1) * HD],
                        preferred_element_type=jnp.float32,
                    )
                else:
                    top = jnp.maximum(top, tops[head])
                    fade = jnp.exp2(tops[head] - top)
                    weights = jnp.exp2(scores - top)
                    sums[head] = sums[head] * fade + jnp.sum(weights, axis=1, keepdims=True)
                    accs[head] = accs[head] * fade + jnp.dot(
                        weights.astype(jnp.bfloat16), kvs[piece][:, width + head * HD : width + (head + 1) * HD],
                        preferred_element_type=jnp.float32,
                    )
                tops[head] = top

        if piece == 0:
            visit()
        else:
            pl.when((base <= first + rows - 1) & (base + piece_rows > lowest))(visit)

    for head in range(heads):
        out[:, head * HD : (head + 1) * HD] = (accs[head] / sums[head]).astype(jnp.bfloat16)


def attend(queries, starts, lowest, first, kvs, bases):
    count, width = queries.shape
    heads = width // HD
    rows = min(256, count)
    steps = count // rows
    info = jnp.concatenate([jnp.stack([first]), lowest, jnp.stack(bases)]).astype(jnp.int32)
    grid_spec = pltpu.PrefetchScalarGridSpec(
        num_scalar_prefetch=1,
        grid=(steps,),
        in_specs=[
            pl.BlockSpec((rows, width), lambda i, _: (i, 0)),
            pl.BlockSpec((rows, 1), lambda i, _: (i, 0)),
        ]
        + [pl.BlockSpec(kv.shape, lambda i, _: (0, 0)) for kv in kvs],
        out_specs=pl.BlockSpec((rows, width), lambda i, _: (i, 0)),
        scratch_shapes=[
            pltpu.VMEM((heads, rows, 1), jnp.float32),
            pltpu.VMEM((heads, rows, 1), jnp.float32),
            pltpu.VMEM((heads, rows, HD), jnp.float32),
        ],
    )
    return pl.pallas_call(
        functools.partial(attend_body, pieces=len(kvs), rows=rows, heads=heads),
        grid_spec=grid_spec,
        out_shape=jax.ShapeDtypeStruct((count, width), jnp.bfloat16),
        name=f"attend{len(kvs)}",
    )(info, queries, starts, *kvs)


def shards(
    failed_section,
    token_ids,
    section_outputs,
    w_query,
    w_key,
    w_value,
    w_out,
    m_value,
    v_value,
    m_out,
    v_out,
):
    replicas = lax.axis_size("dp")
    sections = lax.axis_size("section")
    tensors = lax.axis_size("tensor")
    replica = lax.axis_index("dp")
    section = lax.axis_index("section")
    tensor = lax.axis_index("tensor")
    failed = jnp.remainder(failed_section[0], sections)
    replacing = section == failed
    core = section % 2
    own_side = (failed % 2) == core

    states = [a[0] for a in (w_query, w_key, w_value, w_out, m_value, v_value, m_out, v_out)]
    shard_rows, inner_local = states[0].shape
    model = shard_rows * replicas
    narrow = [a.astype(jnp.bfloat16) for a in states]

    def from_replicas(array):
        return [passed_along(array, "dp", k) for k in range(1, replicas)]

    def whole_rows(own, others):
        full = jnp.zeros((model,) + own.shape[1:], own.dtype)
        for k, part in enumerate([own] + others):
            at = jnp.remainder(replica - k, replicas) * shard_rows
            full = lax.dynamic_update_slice(full, part, (at, 0))
        return full

    others = [None] * 8
    w_in = jnp.concatenate(narrow[:3], axis=1)
    in_others = from_replicas(w_in)
    for k in range(3):
        others[k] = [o[:, k * inner_local : (k + 1) * inner_local] for o in in_others]
    for k in range(3, 8):
        others[k] = from_replicas(narrow[k])

    w_in_full = whole_rows(w_in, in_others)
    w_in_used = jnp.where(own_side, w_in_full, swapped(w_in_full))
    w_out_full = whole_rows(narrow[3], others[3])
    w_out_used = jnp.where(own_side, w_out_full, swapped(w_out_full))

    x_own = section_outputs[0, 0]
    token_count, feats = x_own.shape
    w_steps = [
        lax.dynamic_slice_in_dim(w_in_used, jnp.remainder(tensor - k, tensors) * feats, feats, 0)
        for k in range(tensors)
    ]
    out_steps = []
    for k in range(tensors):
        part = lax.dynamic_slice_in_dim(w_out_used, jnp.remainder(tensor + k, tensors) * feats, feats, 0)
        out_steps.append(passed_along(part, "tensor", k) if k else part)

    starts = document_starts(token_ids[0])
    sub = token_count // (2 * CHUNKS)
    rows = min(256, sub)

    def sub_rows(array, index):
        return lax.dynamic_slice_in_dim(array, index * sub, sub, 0)

    kvs, bases, updates = [], [], []
    for chunk in range(CHUNKS):
        mine, other = 2 * chunk + core, 2 * chunk + 1 - core
        near = passed_along(sub_rows(x_own, other), "section", 1)
        far = lax.ppermute(
            x_own[(2 * chunk + 1) * sub : (2 * chunk + 2) * sub],
            "section",
            [(i, (i + 2) % sections) for i in range(1, sections, 2)],
        )
        piece = jnp.where(
            failed % 2 == 1,
            jnp.where(core == 0, sub_rows(x_own, mine), near),
            jnp.where(core == 0, near, far),
        )
        projected = jnp.dot(piece, w_steps[0], preferred_element_type=jnp.float32)
        for k in range(1, tensors):
            piece = passed_along(piece, "tensor", 1)
            projected = projected + jnp.dot(piece, w_steps[k], preferred_element_type=jnp.float32)
        projected = projected.astype(jnp.bfloat16)
        kv = projected[:, inner_local:]
        kv_other = swapped(kv)
        first = mine * sub
        my_starts = sub_rows(starts, mine)
        lowest = my_starts.reshape(sub // rows, rows)[:, 0]
        context = attend(
            projected[:, :inner_local],
            my_starts[:, None],
            lowest,
            first,
            [kv, kv_other] + kvs,
            [first, other * sub] + bases,
        )
        kvs = kvs + [kv, kv_other]
        bases = bases + [first, other * sub]
        update = jnp.zeros((), jnp.float32)
        for k in range(tensors):
            if k:
                context = passed_along(context, "tensor", 1)
            update = update + lax.dot_general(
                context, out_steps[k], (((1,), (1,)), ((), ())), preferred_element_type=jnp.float32
            )
        update = update.astype(jnp.bfloat16)
        update_other = swapped(update)
        updates.append(jnp.where(core == 0, update, update_other))
        updates.append(jnp.where(core == 0, update_other, update))

    update = jnp.concatenate(updates, axis=0)
    update_block = jnp.where(replacing, update, jnp.zeros_like(update))[None, None]

    def placed(own, parts):
        full = whole_rows(own, [p.astype(jnp.float32) for p in parts])
        return jnp.where(replacing, full, jnp.zeros_like(full))[None, None]

    return tuple(placed(states[k], others[k]) for k in range(8)) + (update_block,)


def solution(mesh):
    state = P("section", "dp", "tensor")
    block = P("dp", "section", None, "tensor")
    return jax.shard_map(
        shards,
        mesh=mesh,
        in_specs=(P("dp"), P("dp", None), block) + (state,) * 8,
        out_specs=(block,) * 9,
        check_vma=False,
    )
```
